256 devices in a mesh: img: 16 (over z, core), pix: 16 (over x, y).
Axes of the slice: x: 4, y: 4, z: 8, core: 2. Of those that a mesh axis runs over, the one named last changes fastest.
Arguments:
- images: bfloat16 [51200, 16384], P('img', 'pix'), may hold values from -6 to 6
- classes: int32 [51200], P('img'), may hold values from 0 to 63
- ctf_table: bfloat16 [64, 16384], P(None, 'pix'), may hold values from -1 to 1, as said below
- weights: float32 [51200], P('img'), may hold values from 0.1 to 1
- probes: float32 [16384, 256], P('pix'), may hold values from -6 to 6
Outputs:
- basis: float32 [16384, 256], P('pix')
- factor: float32 [256, 256], replicated
The draws below stay inside these ranges and needn't reach their ends.
Inputs may be any that keep to these rules, and one draw needn't show every extreme that they name: `ctf_table`: a smooth envelope over the pixel index times an independent magnitude and sign for each entry.
All inputs are finite; a program needn't handle non-finite values.
Results may differ from the reference program's by a relative error of at most 0.012.
Values may be sent and summed in bfloat16 or wider, within the bound.
A program may use at most 64 MiB of HBM per device.

```python
import math
import jax
import jax.numpy as jnp
from jax import lax

PIXELS = 16384
R = 256
CLASSES = 64
ITERS = 2
IMAGES = 51200


def draw_ctf_table(key, part):
    first_key = jax.random.fold_in(key, 11)
    second_key = jax.random.fold_in(key, 12)
    position = jnp.arange(PIXELS).astype(jnp.float32) / PIXELS
    envelope = jnp.exp(-1.5 * position)
    magnitude = jax.random.uniform(first_key, (CLASSES, PIXELS), jnp.float32, 0.3, 1.0)
    signs = jnp.where(jax.random.bernoulli(second_key, 0.5, (CLASSES, PIXELS)), 1.0, -1.0)
    return (envelope[None, :] * magnitude * signs).astype(jnp.bfloat16)


def plant(array, key, low, high):
    place = [jax.random.randint(jax.random.fold_in(key, axis), (), 0, length) for axis, length in enumerate(array.shape)]
    widest = array.shape.index(max(array.shape))
    next_to = place[:widest] + [(place[widest] + 1) % array.shape[widest]] + place[widest + 1:]
    return array.at[tuple(place)].set(low).at[tuple(next_to)].set(high)


def level_of(rng, extent, shards, least, top_value):
    gain, own = 1.0, jax.random.fold_in(rng, 6)
    for axis_at, shards_of in shards:
        draws = jnp.exp(jax.random.uniform(jax.random.fold_in(own, axis_at), (shards_of,), jnp.float32, least / len(shards), top_value / len(shards)))
        gain = gain * jnp.repeat(draws, extent[axis_at] // shards_of).reshape([-1 if axis == axis_at else 1 for axis in range(len(extent))])
    return gain


def normal_values(stream_key, extent, scale, most, split=(), dtype=jnp.bfloat16):
    array = jax.random.normal(stream_key, extent, jnp.float32) * scale
    if len(split) > 0:
        array = level_of(stream_key, extent, split, -0.22, 0.18) * array
    return jnp.clip(array, min=-most, max=most).astype(dtype)


def setup_inputs(seed: int = 0) -> dict:
    arg_keys = jax.random.split(jax.random.key(seed), 6)
    images = normal_values(arg_keys[0], (IMAGES, PIXELS), 1.0, 6.0, ((0, 16), (1, 16)))
    classes = plant(jax.random.randint(arg_keys[1], (IMAGES,), 0, CLASSES), jax.random.fold_in(arg_keys[1], 1), 0, CLASSES - 1).astype(jnp.int32)
    ctf_table = draw_ctf_table(jax.random.fold_in(arg_keys[5], 71), 0)
    weights = jnp.clip(jnp.exp(math.log(1.0) - 2.3025851 * jax.random.uniform(arg_keys[3], (IMAGES,), jnp.float32) ** level_of(arg_keys[3], (IMAGES,), ((0, 16),), -0.2, 0.2)), 0.1, 1.0)
    probes = normal_values(arg_keys[4], (PIXELS, R), 1.0, 6.0, ((0, 16),), jnp.float32)
    return {"images": images, "classes": classes, "ctf_table": ctf_table, "weights": weights, "probes": probes}


def reference(images, classes, ctf_table, weights, probes):
    filters = ctf_table[classes].astype(jnp.float32)
    filtered = (images.astype(jnp.float32) * filters).astype(jnp.bfloat16)
    current = probes
    factor = jnp.zeros((R, R), jnp.float32)
    for sweep in range(ITERS):
        probe_half = current.astype(jnp.bfloat16)
        scores = jnp.dot(filtered.astype(jnp.float32), probe_half.astype(jnp.float32), preferred_element_type=jnp.float32)
        scaled = (weights[:, None] * scores).astype(jnp.bfloat16)
        image_sum = jnp.dot(filtered.T.astype(jnp.float32), scaled.astype(jnp.float32), preferred_element_type=jnp.float32)
        gram_matrix = jnp.dot(image_sum.T, image_sum, precision=lax.Precision.HIGHEST)
        factor = jnp.linalg.cholesky(gram_matrix)
        current = jax.scipy.linalg.solve_triangular(factor, image_sum.T, lower=True).T
    return (current, factor)
```

```python
import jax
import jax.numpy as jnp
from jax import lax
from jax.experimental import pallas as pl
from jax.experimental.pallas import tpu as pltpu
from jax.sharding import Mesh
from jax.sharding import PartitionSpec as P

ITERS = 2
IMG = ("img_0", "img_1")

HIGHEST = lax.Precision.HIGHEST
UP = float(2.0**24)
DOWN = float(2.0**-24)

def product(a, b, dims=((1,), (0,))):
    return lax.dot_general(a, b, (dims, ((), ())), precision=HIGHEST, preferred_element_type=jnp.float32)


def factor_blocks(gram, work, spread, small, inverse, upper):
    pair, n = gram.shape[0], gram.shape[1]
    work[...] = gram[...]
    lane = lax.broadcasted_iota(jnp.int32, (pair, 128), 1)
    col = lax.broadcasted_iota(jnp.int32, (16, n), 1)
    for start in range(0, n, 16):
        chunk = start // 128 * 128
        off = start - chunk
        for g in range(pair):
            block = work[g, start : start + 16, chunk : chunk + 128]
            for j in range(16):
                spread[j, 16 * g : 16 * g + 16, :] = jnp.broadcast_to(block[:, off + j : off + j + 1], (16, 128))
        a = {(i, j): spread[j, pl.ds(i, pair, stride=16), :] for j in range(16) for i in range(j, 16)}
        inv = []
        t = {}
        for j in range(16):
            root = lax.rsqrt(a[j, j])
            inv.append(root)
            for i in range(j + 1, 16):
                a[i, j] = a[i, j] * root
            for m in range(j + 1, 16):
                for i in range(m, 16):
                    a[i, m] = a[i, m] - a[i, j] * a[m, j]
            t[j, j] = root
            row = jnp.where(lane == off + j, root, 0.0)
            for m in range(j):
                total = a[j, m] * t[m, m]
                for q in range(m + 1, j):
                    total = total + a[j, q] * t[q, m]
                t[j, m] = -root * total
                row = jnp.where(lane == off + m, t[j, m], row)
            small[pl.ds(j, pair, stride=16), :] = row
        for g in range(pair):
            head = small[16 * g : 16 * g + 16, :]
            lead = product(head, work[g, chunk : chunk + 128, :])
            wide = jnp.concatenate([head, head], axis=1) if n == 256 else head
            here = (col >= start) & (col < start + 16)
            mixed = jnp.where(here, wide, lead)
            inverse[g, start : start + 16, :] = jnp.where(col < start + 16, mixed, 0.0)
            upper[g, start : start + 16, :] = jnp.where(
                col >= start + lax.broadcasted_iota(jnp.int32, (16, n), 0), lead, 0.0)
            below = start + 16
            if below < n:
                side = product(work[g, below:, chunk : chunk + 128], head, ((1,), (1,)))
                cols = lax.broadcasted_iota(jnp.int32, (n - below, n), 1)
                old = work[g, below:, :]
                old = jnp.where((cols >= start) & (cols < below), 0.0, old)
                work[g, below:, :] = old - product(side, mixed)


def finish_kernel(image_sum, gram, basis, factor, work, spread, small, inverse, upper):
    factor_blocks(gram, work, spread, small, inverse, upper)
    basis[...] = product(image_sum[...].astype(jnp.float32), inverse[1], ((1,), (1,)))
    factor[...] = UP * product(inverse[0], upper[1], ((1,), (1,)))


def finish(image_sum, gram):
    rows, n = image_sum.shape
    return pl.pallas_call(
        finish_kernel,
        out_shape=(jax.ShapeDtypeStruct((rows, n), jnp.float32), jax.ShapeDtypeStruct((n, n), jnp.float32)),
        in_specs=[pl.BlockSpec(memory_space=pltpu.VMEM)] * 2,
        out_specs=[pl.BlockSpec(memory_space=pltpu.VMEM)] * 2,
        scratch_shapes=[
            pltpu.VMEM((2, n, n), jnp.float32),
            pltpu.VMEM((16, 32, 128), jnp.float32),
            pltpu.VMEM((32, 128), jnp.float32),
            pltpu.VMEM((2, n, n), jnp.float32),
            pltpu.VMEM((2, n, n), jnp.float32),
        ],
    )(image_sum, gram)


def cut_along(x, dim, devices):
    before, after = (x.shape[:dim], x.shape[dim + 1 :])
    return jnp.moveaxis(x.reshape(*before, devices, -1, *after), dim, 0)


def summed_on_arrival(x, axis, dim):
    blocks = cut_along(x, dim, lax.axis_size(axis))
    arrived = lax.all_to_all(blocks, axis, split_axis=0, concat_axis=0, tiled=True)
    return arrived.astype(jnp.float32).sum(axis=0)


def sent_to_all(x, axis):
    devices = lax.axis_size(axis)
    return lax.all_to_all(jnp.broadcast_to(x[None], (devices, *x.shape)), axis, 0, 0, tiled=True)


def joined_along(blocks, dim):
    lengths = list(blocks.shape[1:])
    lengths[dim] *= blocks.shape[0]
    return jnp.moveaxis(blocks, 0, dim).reshape(lengths)


def collect(x, axis, dim):
    blocks = sent_to_all(x, axis)
    return joined_along(blocks, dim)


def sum_in_two_steps(x, axes, dim):
    far, near = axes
    own = summed_on_arrival(cut_along(x, dim, lax.axis_size(far)), near, dim + 1)
    return jnp.sum(
        lax.all_to_all(own.astype(jnp.bfloat16), far, 0, 0, tiled=True).astype(jnp.float32), axis=0
    )


def rows_for(lines, devices):
    spare = -lines.shape[0] % devices
    if not spare:
        return lines
    return jnp.concatenate([lines, jnp.zeros((spare, *lines.shape[1:]), lines.dtype)])


def gather_axes(x, axes, dim):
    far, near = axes
    blocks = sent_to_all(sent_to_all(x, far), near)
    return joined_along(blocks.swapaxes(0, 1).reshape(-1, *x.shape), dim)


def sum_by_parts(x, axes):
    lines = x.reshape(-1, x.shape[-1])
    own = sum_in_two_steps(
        rows_for(lines, lax.axis_size(axes[0]) * lax.axis_size(axes[1])), axes, 0
    )
    whole = gather_axes(own.astype(jnp.bfloat16), axes, 0)
    return whole[: len(lines)].reshape(x.shape).astype(jnp.float32)


def summed_on_arrival_2(x, axis, dim):
    devices = lax.axis_size(axis)
    blocks = lax.all_to_all(cut_along(x, dim, devices), axis, 0, 0, tiled=True)
    return jnp.sum(blocks, axis=0)


def sum_by_parts_2(x, axes):
    lines = x.reshape(-1, x.shape[-1])
    padded = rows_for(lines, lax.axis_size(axes))
    whole = collect(summed_on_arrival_2(padded, axes, 0), axes, 0)
    return lax.slice_in_dim(whole, 0, len(lines)).reshape(x.shape)


def power_step(filtered, weight_share, probe_half):
    shares = summed_on_arrival(
        jnp.dot(filtered, probe_half, preferred_element_type=jnp.float32).astype(jnp.bfloat16),
        "pix",
        0,
    )
    scaled_share = (weight_share[:, None] * shares).astype(jnp.bfloat16)
    scaled = collect(scaled_share, "pix", 0)
    partial_sum = lax.dot_general(
        filtered, scaled, (((0,), (0,)), ((), ())), preferred_element_type=jnp.float32
    )
    return sum_by_parts(partial_sum.astype(jnp.bfloat16), ("img_0", "img_1"))


def per_device(images, classes, ctf_table, weights, probes):
    onehot = (classes[:, None] == jnp.arange(ctf_table.shape[0])[None, :]).astype(jnp.bfloat16)
    filters = jnp.dot(onehot, ctf_table, preferred_element_type=jnp.float32)
    filtered = (images.astype(jnp.float32) * filters).astype(jnp.bfloat16)
    share_rows = filtered.shape[0] // lax.axis_size("pix")
    weight_share = lax.dynamic_slice_in_dim(
        weights, lax.axis_index("pix") * share_rows, share_rows, 0
    )
    first = power_step(filtered, weight_share, probes.astype(jnp.bfloat16))
    second = power_step(filtered, weight_share, (first * DOWN).astype(jnp.bfloat16))
    grams = jnp.stack([jnp.dot(s.T, s, precision=HIGHEST) for s in (first, second)])
    gram = sum_by_parts_2(grams, "pix")
    return finish(second, gram)


def solution(mesh):
    split = Mesh(mesh.devices.reshape(8, 2, mesh.shape["pix"]), ("img_0", "img_1", "pix"))
    return jax.shard_map(
        per_device,
        mesh=split,
        in_specs=(P(IMG, "pix"), P(IMG), P(None, "pix"), P(IMG), P("pix", None)),
        out_specs=(P("pix", None), P()),
        check_vma=False,
    )
```

```python
import jax
import jax.numpy as jnp
from jax import lax
from jax.experimental import pallas as pl
from jax.experimental.pallas import tpu as pltpu
from jax.sharding import PartitionSpec as P

ITERS = 2

HIGHEST = lax.Precision.HIGHEST
UP = float(2.0**24)
DOWN = float(2.0**-24)

def product(a, b, dims=((1,), (0,))):
    return lax.dot_general(a, b, (dims, ((), ())), precision=HIGHEST, preferred_element_type=jnp.float32)


def factor_blocks(gram, work, spread, small, inverse, upper):
    pair, n = gram.shape[0], gram.shape[1]
    work[...] = gram[...]
    lane = lax.broadcasted_iota(jnp.int32, (pair, 128), 1)
    col = lax.broadcasted_iota(jnp.int32, (16, n), 1)
    for start in range(0, n, 16):
        chunk = start // 128 * 128
        off = start - chunk
        for g in range(pair):
            block = work[g, start : start + 16, chunk : chunk + 128]
            for j in range(16):
                spread[j, 16 * g : 16 * g + 16, :] = jnp.broadcast_to(block[:, off + j : off + j + 1], (16, 128))
        a = {(i, j): spread[j, pl.ds(i, pair, stride=16), :] for j in range(16) for i in range(j, 16)}
        inv = []
        t = {}
        for j in range(16):
            root = lax.rsqrt(a[j, j])
            inv.append(root)
            for i in range(j + 1, 16):
                a[i, j] = a[i, j] * root
            for m in range(j + 1, 16):
                for i in range(m, 16):
                    a[i, m] = a[i, m] - a[i, j] * a[m, j]
            t[j, j] = root
            row = jnp.where(lane == off + j, root, 0.0)
            for m in range(j):
                total = a[j, m] * t[m, m]
                for q in range(m + 1, j):
                    total = total + a[j, q] * t[q, m]
                t[j, m] = -root * total
                row = jnp.where(lane == off + m, t[j, m], row)
            small[pl.ds(j, pair, stride=16), :] = row
        for g in range(pair):
            head = small[16 * g : 16 * g + 16, :]
            lead = product(head, work[g, chunk : chunk + 128, :])
            wide = jnp.concatenate([head, head], axis=1) if n == 256 else head
            here = (col >= start) & (col < start + 16)
            mixed = jnp.where(here, wide, lead)
            inverse[g, start : start + 16, :] = jnp.where(col < start + 16, mixed, 0.0)
            upper[g, start : start + 16, :] = jnp.where(
                col >= start + lax.broadcasted_iota(jnp.int32, (16, n), 0), lead, 0.0)
            below = start + 16
            if below < n:
                side = product(work[g, below:, chunk : chunk + 128], head, ((1,), (1,)))
                cols = lax.broadcasted_iota(jnp.int32, (n - below, n), 1)
                old = work[g, below:, :]
                old = jnp.where((cols >= start) & (cols < below), 0.0, old)
                work[g, below:, :] = old - product(side, mixed)


def finish_kernel(image_sum, gram, basis, factor, work, spread, small, inverse, upper):
    factor_blocks(gram, work, spread, small, inverse, upper)
    basis[...] = product(inverse[1], image_sum[...].astype(jnp.float32)).T
    factor[...] = product(inverse[0], upper[1], ((1,), (1,)))


def finish(image_sum, gram):
    n, rows = image_sum.shape
    return pl.pallas_call(
        finish_kernel,
        out_shape=(jax.ShapeDtypeStruct((rows, n), jnp.float32), jax.ShapeDtypeStruct((n, n), jnp.float32)),
        in_specs=[pl.BlockSpec(memory_space=pltpu.VMEM)] * 2,
        out_specs=[pl.BlockSpec(memory_space=pltpu.VMEM)] * 2,
        scratch_shapes=[
            pltpu.VMEM((2, n, n), jnp.float32),
            pltpu.VMEM((16, 32, 128), jnp.float32),
            pltpu.VMEM((32, 128), jnp.float32),
            pltpu.VMEM((2, n, n), jnp.float32),
            pltpu.VMEM((2, n, n), jnp.float32),
        ],
    )(image_sum, gram)


SHARE_TILES = ((7, 6, 6, 6), (6, 6, 7, 6))
WIDTH = 128
MESH = pl.DeviceIdType.MESH


def remote(src, dst, send, recv, to):
    return pltpu.make_async_remote_copy(
        src_ref=src, dst_ref=dst, send_sem=send, recv_sem=recv, device_id=to, device_id_type=MESH)


class Place:
    def __init__(self):
        self.img, self.pix = lax.axis_index("img"), lax.axis_index("pix")
        self.z, self.core = self.img // 2, self.img % 2
        x, y = self.pix // 4, self.pix % 4
        self.bits, self.across = [], []
        for near, far in ((x, y), (y, x)):
            high, low = near // 2, near % 2
            self.bits.append(((high + low) % 2, high))
        flips = ((x + 1 - 2 * (x % 2)) * 4 + y, (3 - x) * 4 + y, x * 4 + y + 1 - 2 * (y % 2), x * 4 + 3 - y)
        (xv, xu), (yv, yu) = self.bits
        self.bits = (xv, yv, xu, yu)
        self.across = tuple((self.img, p) for p in (flips[0], flips[2], flips[1], flips[3]))
        self.partner = (self.z * 2 + 1 - self.core, self.pix)

    def along_z(self, d):
        return ((self.z + d) % 8 * 2 + self.core, self.pix)

    def in_plane(self, d):
        return (self.img, (self.pix + d) % 16)


def greet(here):
    barrier = pltpu.get_barrier_semaphore()
    peers = [here.in_plane(d) for d in range(1, 16)] + [here.along_z(d) for d in range(1, 8)] + [here.partner]
    for peer in peers:
        pl.semaphore_signal(barrier, inc=1, device_id=peer, device_id_type=MESH)
    pl.semaphore_wait(barrier, len(peers))


def tiles_of(c):
    first, streams = 0, []
    for share in SHARE_TILES[c]:
        streams.append((first, share))
        first += 16 * share
    return streams


def sweep(here, sends, t, c, filtered, weights, probe, scores, landed, scaled, shares, crossed, halves, arrived, whole, sems):
    rs_send, rs_recv, ag_send, ag_recv, d2d_send, d2d_recv, z_send, z_recv, g_send, g_recv, f_send, f_recv = sems
    streams = tiles_of(c)
    dims = ((1,), (0,)) if t == 0 else ((1,), (1,))

    def bit(s, i):
        return here.bits[(s + i) % 4]

    def across(s, i):
        return here.across[(s + i) % 4]

    start = [[first] for first, _ in streams]
    flow = [[None] * 4 for _ in streams]
    base = 0

    def score(first, tiles):
        rows = pl.ds(pl.multiple_of(first * 8, 64), tiles * 8)
        part = lax.dot_general(
            filtered[rows, :], probe(), (dims, ((), ())), preferred_element_type=jnp.float32)
        scores[pl.ds(first, tiles)] = part.reshape(tiles, 8, WIDTH).astype(jnp.bfloat16)

    def pass_half(s, i):
        share = streams[s][1]
        half = share * 16 >> (i + 1)
        off = start[s][i]
        give, keep = off + (1 - bit(s, i)) * half, off + bit(s, i) * half
        start[s].append(keep)
        return give, keep, half

    slots = []
    at = 0
    for i in range(4):
        for s in range(4):
            slots.append(at)
            at += streams[s][1] * 16 >> (i + 1)

    def send_half(s, i, give, half):
        flow[s][i] = remote(
            scores.at[pl.ds(give, half)], landed.at[pl.ds(slots[4 * i + s], half)],
            rs_send.at[i, s], rs_recv.at[i, s], across(s, i))
        flow[s][i].start()
        sends.append(flow[s][i])

    todo = []
    for s in range(4):
        give, keep, half = pass_half(s, 0)
        score(give, half)
        send_half(s, 0, give, half)
        todo.append((keep, half))
    for keep, half in todo:
        score(keep, half)
    for i in range(4):
        yield ("rs", t, i)
        for s in range(4):
            half = streams[s][1] * 16 >> (i + 1)
            keep = start[s][i + 1]
            flow[s][i].wait_recv()
            mine = scores[pl.ds(keep, half)].astype(jnp.float32)
            mine = mine + landed[pl.ds(slots[4 * i + s], half)].astype(jnp.float32)
            if i < 3:
                scores[pl.ds(keep, half)] = mine.astype(jnp.bfloat16)
                give, _, small = pass_half(s, i + 1)
                send_half(s, i + 1, give, small)
            else:
                scaled[pl.ds(keep, half)] = (weights[pl.ds(keep, half)] * mine).astype(jnp.bfloat16)
                flow[s][3] = None
    back = [[None] * 4 for _ in streams]

    def send_back(s, i):
        half = streams[s][1] * 16 >> (i + 1)
        own = scaled.at[pl.ds(start[s][i + 1], half)]
        back[s][i] = remote(own, own, ag_send.at[i, s], ag_recv.at[i, s], across(s, i))
        back[s][i].start()
        sends.append(back[s][i])

    for s in range(4):
        send_back(s, 3)
    for i in (3, 2, 1, 0):
        yield ("ag", t, 3 - i)
        for s in range(4):
            back[s][i].wait_recv()
            if i:
                send_back(s, i - 1)
    total = lax.dot_general(
        scaled[...].reshape(-1, WIDTH), filtered[...], (((0,), (0,)), ((), ())), preferred_element_type=jnp.float32)
    shares[...] = total.reshape(16, 8, -1).astype(jnp.bfloat16)
    swap = remote(shares.at[pl.ds((1 - here.core) * 8, 8)], crossed, d2d_send.at[0], d2d_recv.at[0], here.partner)
    swap.start()
    sends.append(swap)
    yield ("img", t, 0)
    swap.wait_recv()
    rounds = []
    for d in range(1, 8):
        k = (here.z + d) % 8
        pair = shares[here.core * 8 + k].astype(jnp.float32) + crossed[k].astype(jnp.float32)
        halves[d] = pair.astype(jnp.bfloat16)
        copy = remote(halves.at[d], arrived.at[d], z_send.at[d], z_recv.at[d], here.along_z(d))
        copy.start()
        rounds.append(copy)
    sends.extend(rounds)
    own = shares[here.core * 8 + here.z].astype(jnp.float32) + crossed[here.z].astype(jnp.float32)
    yield ("img", t, 1)
    for d, copy in enumerate(rounds, 1):
        copy.wait_recv()
        own = own + arrived[d].astype(jnp.float32)
    mine = here.core * 8 + here.z
    whole[mine] = own.astype(jnp.bfloat16)
    rounds = []
    for d in range(1, 8):
        copy = remote(whole.at[mine], whole.at[mine], g_send.at[d], g_recv.at[d], here.along_z(d))
        copy.start()
        rounds.append(copy)
    sends.extend(rounds)
    over = [remote(whole.at[mine], whole.at[mine], f_send.at[0], f_recv.at[0], here.partner)]
    over[0].start()
    yield ("img", t, 2)
    for d, copy in enumerate(rounds, 1):
        copy.wait_recv()
        k = here.core * 8 + (here.z + 8 - d) % 8
        fwd = remote(whole.at[k], whole.at[k], f_send.at[d], f_recv.at[d], here.partner)
        fwd.start()
        over.append(fwd)
    sends.extend(over)
    yield ("img", t, 3)
    for fwd in over:
        fwd.wait_recv()


def gram_sum(here, sends, basis, out, parts, landed, sems):
    r_send, r_recv, a_send, a_recv = sems
    gram = lax.dot_general(basis[...], basis[...], (((1,), (1,)), ((), ())), preferred_element_type=jnp.float32)
    parts[...] = gram.reshape(16, 16, -1)
    rounds = []
    for d in range(1, 16):
        copy = remote(parts.at[(here.pix + d) % 16], landed.at[d], r_send.at[d], r_recv.at[d], here.in_plane(d))
        copy.start()
        rounds.append(copy)
    sends.extend(rounds)
    own = parts[here.pix]
    yield ("gram", 0, 0)
    for d, copy in enumerate(rounds, 1):
        copy.wait_recv()
        own = own + landed[d]
    out[here.pix] = own
    rounds = []
    for d in range(1, 16):
        copy = remote(out.at[here.pix], out.at[here.pix], a_send.at[d], a_recv.at[d], here.in_plane(d))
        copy.start()
        rounds.append(copy)
    sends.extend(rounds)
    yield ("gram", 0, 1)
    for copy in rounds:
        copy.wait_recv()


def sweeps_kernel(
    filtered, weights, probes, basis, grams,
    scores, landed, scaled, shares, crossed, halves, arrived, whole, joined, parts, gram_landed, gram_whole,
    rs_send, rs_recv, ag_send, ag_recv, d2d_send, d2d_recv, z_send, z_recv, g_send, g_recv, f_send, f_recv,
    r_send, r_recv, a_send, a_recv,
):
    here = Place()
    greet(here)
    sends = []
    all_sems = (rs_send, rs_recv, ag_send, ag_recv, d2d_send, d2d_recv, z_send, z_recv, g_send, g_recv, f_send, f_recv)

    def run(c):
        cols = slice(c * WIDTH, (c + 1) * WIDTH)
        for t in range(ITERS):
            probe = (lambda: probes[:, cols]) if t == 0 else (lambda: joined[0, cols, :])
            n = 2 * t + c
            yield from sweep(
                here, sends, t, c, filtered, weights, probe, scores.at[n], landed.at[n], scaled.at[n], shares.at[n],
                crossed.at[n], halves.at[n], arrived.at[n], whole.at[n], [sem.at[n] for sem in all_sems])
            found = whole[n].reshape(WIDTH, -1)
            if t == 0:
                joined[0, cols, :] = (found.astype(jnp.float32) * DOWN).astype(jnp.bfloat16)
            else:
                basis[cols, :] = found

    def gram(t):
        sems = [sem.at[t] for sem in (r_send, r_recv, a_send, a_recv)]
        yield from gram_sum(
            here, sends, joined.at[0] if t == 0 else basis, gram_whole.at[t], parts.at[t], gram_landed.at[t], sems)

    live = [run(c) for c in range(2)]
    label = next(live[0])
    while label != LAG:
        label = next(live[0])
    pending = True
    while live:
        for one in list(live):
            label = next(one, None)
            if label is None:
                live.remove(one)
            elif label == ("img", 1, 0) and pending and one is live[-1]:
                pending = False
                live.append(gram(0))
    for _ in gram(1):
        pass
    grams[...] = gram_whole[...]
    for copy in sends:
        copy.wait_send()


LAG = ("rs", 0, 0)


def sweeps(filtered, weights, probes):
    rows, pixels = filtered.shape
    n = probes.shape[1]
    tiles = rows // 8
    four = 2 * ITERS
    bf16, f32 = jnp.bfloat16, jnp.float32
    dma = pltpu.SemaphoreType.DMA
    vmem = pl.BlockSpec(memory_space=pltpu.VMEM)
    return pl.pallas_call(
        sweeps_kernel,
        out_shape=(jax.ShapeDtypeStruct((n, pixels), bf16), jax.ShapeDtypeStruct((2, 16, 16, n), f32)),
        in_specs=[vmem] * 3,
        out_specs=[vmem] * 2,
        scratch_shapes=[
            pltpu.VMEM((four, tiles, 8, WIDTH), bf16),
            pltpu.VMEM((four, tiles * 15 // 16, 8, WIDTH), bf16),
            pltpu.VMEM((four, tiles, 8, WIDTH), bf16),
            pltpu.VMEM((four, 16, 8, pixels), bf16),
            pltpu.VMEM((four, 8, 8, pixels), bf16),
            pltpu.VMEM((four, 8, 8, pixels), bf16),
            pltpu.VMEM((four, 8, 8, pixels), bf16),
            pltpu.VMEM((four, 16, 8, pixels), bf16),
            pltpu.VMEM((1, n, pixels), bf16),
            pltpu.VMEM((2, 16, 16, n), f32),
            pltpu.VMEM((2, 16, 16, n), f32),
            pltpu.VMEM((2, 16, 16, n), f32),
            *[dma((four, 4, 4))] * 4,
            *[dma((four, 1))] * 2,
            *[dma((four, 8))] * 6,
            *[dma((2, 16))] * 4,
        ],
        compiler_params=pltpu.CompilerParams(
            collective_id=0, has_side_effects=True, vmem_limit_bytes=56 * 2**20),
    )(filtered, weights, probes)


def per_device(images, classes, ctf_table, weights, probes):
    onehot = (classes[:, None] == jnp.arange(ctf_table.shape[0])[None, :]).astype(jnp.bfloat16)
    filters = jnp.dot(onehot, ctf_table, preferred_element_type=jnp.float32)
    filtered = (images.astype(jnp.float32) * filters).astype(jnp.bfloat16)
    spread = jnp.broadcast_to(weights.reshape(-1, 8, 1), (weights.shape[0] // 8, 8, WIDTH))
    image_sum, grams = sweeps(filtered, spread, probes.astype(jnp.bfloat16))
    n = probes.shape[1]
    return finish(image_sum, grams.reshape(2, n, n))


def solution(mesh):
    return jax.shard_map(
        per_device,
        mesh=mesh,
        in_specs=(P("img", "pix"), P("img"), P(None, "pix"), P("img"), P("pix", None)),
        out_specs=(P("pix", None), P()),
        check_vma=False,
    )
```

```python
import jax
import jax.numpy as jnp
from jax import lax
from jax.experimental import pallas as pl
from jax.experimental.pallas import tpu as pltpu
from jax.sharding import PartitionSpec as P

ITERS = 2

HIGHEST = lax.Precision.HIGHEST
UP = float(2.0**24)
DOWN = float(2.0**-24)

def product(a, b, dims=((1,), (0,))):
    return lax.dot_general(a, b, (dims, ((), ())), precision=HIGHEST, preferred_element_type=jnp.float32)


def split(a):
    top = a.astype(jnp.bfloat16)
    return top, (a - top.astype(jnp.float32)).astype(jnp.bfloat16)


def product3(a, b, dims=((1,), (0,))):
    (a0, a1), (b0, b1) = split(a), split(b)

    def one(p, q):
        return lax.dot_general(p, q, (dims, ((), ())), preferred_element_type=jnp.float32)

    return one(a0, b0) + (one(a0, b1) + one(a1, b0))


def factor_blocks(gram, work, spread, small, inverse, upper):
    pair, n = gram.shape[0], gram.shape[1]
    work[...] = gram[...]
    lane = lax.broadcasted_iota(jnp.int32, (pair, 128), 1)
    col = lax.broadcasted_iota(jnp.int32, (16, n), 1)
    for start in range(0, n, 16):
        chunk = start // 128 * 128
        off = start - chunk
        for g in range(pair):
            block = work[g, start : start + 16, chunk : chunk + 128]
            for j in range(16):
                spread[j, 16 * g : 16 * g + 16, :] = jnp.broadcast_to(block[:, off + j : off + j + 1], (16, 128))
        a = {(i, j): spread[j, pl.ds(i, pair, stride=16), :] for j in range(16) for i in range(j, 16)}
        inv = []
        t = {}
        for j in range(16):
            root = lax.rsqrt(a[j, j])
            inv.append(root)
            for i in range(j + 1, 16):
                a[i, j] = a[i, j] * root
            for m in range(j + 1, 16):
                for i in range(m, 16):
                    a[i, m] = a[i, m] - a[i, j] * a[m, j]
            t[j, j] = root
            row = jnp.where(lane == off + j, root, 0.0)
            for m in range(j):
                total = a[j, m] * t[m, m]
                for q in range(m + 1, j):
                    total = total + a[j, q] * t[q, m]
                t[j, m] = -root * total
                row = jnp.where(lane == off + m, t[j, m], row)
            small[pl.ds(j, pair, stride=16), :] = row
        for g in range(pair):
            head = small[16 * g : 16 * g + 16, :]
            lead = product3(head, work[g, chunk : chunk + 128, :])
            wide = jnp.concatenate([head, head], axis=1) if n == 256 else head
            here = (col >= start) & (col < start + 16)
            mixed = jnp.where(here, wide, lead)
            inverse[g, start : start + 16, :] = jnp.where(col < start + 16, mixed, 0.0)
            upper[g, start : start + 16, :] = jnp.where(
                col >= start + lax.broadcasted_iota(jnp.int32, (16, n), 0), lead, 0.0)
            below = start + 16
            if below < n:
                side = product3(work[g, below:, chunk : chunk + 128], head, ((1,), (1,)))
                cols = lax.broadcasted_iota(jnp.int32, (n - below, n), 1)
                old = work[g, below:, :]
                old = jnp.where((cols >= start) & (cols < below), 0.0, old)
                work[g, below:, :] = old - product3(side, mixed)


def finish_kernel(image_sum, gram, basis, factor, work, spread, small, inverse, upper):
    factor_blocks(gram, work, spread, small, inverse, upper)
    basis[...] = product(inverse[1], image_sum[...].astype(jnp.float32)).T
    factor[...] = product(inverse[0], upper[1], ((1,), (1,)))


def finish(image_sum, gram):
    n, rows = image_sum.shape
    return pl.pallas_call(
        finish_kernel,
        out_shape=(jax.ShapeDtypeStruct((rows, n), jnp.float32), jax.ShapeDtypeStruct((n, n), jnp.float32)),
        in_specs=[pl.BlockSpec(memory_space=pltpu.VMEM)] * 2,
        out_specs=[pl.BlockSpec(memory_space=pltpu.VMEM)] * 2,
        scratch_shapes=[
            pltpu.VMEM((2, n, n), jnp.float32),
            pltpu.VMEM((16, 32, 128), jnp.float32),
            pltpu.VMEM((32, 128), jnp.float32),
            pltpu.VMEM((2, n, n), jnp.float32),
            pltpu.VMEM((2, n, n), jnp.float32),
        ],
    )(image_sum, gram)


FLIPS = ((1, 0), (0, 1), (1, 1))
SHARE_TILES = ((7, 6, 6, 6), (6, 6, 7, 6))
WIDTH = 128
MESH = pl.DeviceIdType.MESH


def remote(src, dst, send, recv, to):
    return pltpu.make_async_remote_copy(
        src_ref=src, dst_ref=dst, send_sem=send, recv_sem=recv, device_id=to, device_id_type=MESH)


class Place:
    def __init__(self):
        self.img, self.pix = lax.axis_index("img"), lax.axis_index("pix")
        self.z, self.core = self.img // 2, self.img % 2
        x, y = self.pix // 4, self.pix % 4
        self.x, self.y = x, y
        self.bits = []
        for near, far in ((x, y), (y, x)):
            high, low = near // 2, near % 2
            self.bits.append(((high + low) % 2, high))
        (xv, xu), (yv, yu) = self.bits
        self.bits = (xv, yv, xu, yu)
        self.flipped = (x + 1 - 2 * (x % 2), y + 1 - 2 * (y % 2), 3 - x, 3 - y)
        self.partner = (self.z * 2 + 1 - self.core, self.pix)

    def across(self, *links):
        x, y = self.x, self.y
        for k in links:
            x, y = (x, self.flipped[k]) if k % 2 else (self.flipped[k], y)
        return (self.img, x * 4 + y)

    def along_z(self, d):
        return ((self.z + d) % 8 * 2 + self.core, self.pix)

    def in_plane(self, d):
        return (self.img, (self.pix + d) % 16)


def greet(here):
    barrier = pltpu.get_barrier_semaphore()
    peers = [here.in_plane(d) for d in range(1, 16)] + [here.along_z(d) for d in range(1, 8)] + [here.partner]
    for peer in peers:
        pl.semaphore_signal(barrier, inc=1, device_id=peer, device_id_type=MESH)
    pl.semaphore_wait(barrier, len(peers))


def tiles_of(c):
    first, streams = 0, []
    for share in SHARE_TILES[c]:
        streams.append((first, share))
        first += 16 * share
    return streams


def sweep(here, sends, t, c, prepare, filtered, weights, probe, scores, landed, scaled, shares, crossed, halves, arrived, whole, sems):
    rs_send, rs_recv, ag_send, ag_recv, ws_send, ws_recv, wg_send, wg_recv = sems[:8]
    d2d_send, d2d_recv, z_send, z_recv, g_send, g_recv, f_send, f_recv = sems[8:]
    streams = tiles_of(c)
    dims = ((1,), (0,)) if t == 0 else ((1,), (1,))

    def bit(s, i):
        return here.bits[(s + i) % 4]

    def across(s, i):
        return here.across((s + i) % 4)

    start = [[first] for first, _ in streams]
    flow = [[None] * 4 for _ in streams]
    base = 0

    def score(first, tiles):
        rows = pl.ds(pl.multiple_of(first * 8, 64), tiles * 8)
        part = lax.dot_general(
            filtered[rows, :], probe(), (dims, ((), ())), preferred_element_type=jnp.float32)
        scores[pl.ds(first, tiles)] = part.reshape(tiles, 8, WIDTH).astype(jnp.bfloat16)

    def pass_half(s, i):
        share = streams[s][1]
        half = share * 16 >> (i + 1)
        off = start[s][i]
        give, keep = off + (1 - bit(s, i)) * half, off + bit(s, i) * half
        start[s].append(keep)
        return give, keep, half

    slots = []
    at = 0
    for i in range(2):
        for s in range(4):
            slots.append(at)
            at += streams[s][1] * 16 >> (i + 1)
    for s in range(4):
        slots.append(at)
        at += 3 * streams[s][1]

    def send_half(s, i, give, half):
        flow[s][i] = remote(
            scores.at[pl.ds(give, half)], landed.at[pl.ds(slots[4 * i + s], half)],
            rs_send.at[i, s], rs_recv.at[i, s], across(s, i))
        flow[s][i].start()
        sends.append(flow[s][i])

    def piece(s, flip):
        near, far = (1 - bit(s, i) if f else bit(s, i) for i, f in zip((2, 3), flip))
        return pl.ds(start[s][2] + (2 * near + far) * streams[s][1], streams[s][1])

    def to_three(s, send):
        copies = []
        for j, flip in enumerate(FLIPS):
            links = [(s + i) % 4 for i, f in zip((2, 3), flip) if f]
            copies.append(send(j, flip, here.across(*links)))
            copies[-1].start()
        sends.extend(copies)
        return copies

    def corner(s, j):
        return pl.ds(slots[8 + s] + j * streams[s][1], streams[s][1])

    todo = []
    for s in range(4):
        prepare(s)
        give, keep, half = pass_half(s, 0)
        score(give, half)
        send_half(s, 0, give, half)
        todo.append((keep, half))
    for keep, half in todo:
        score(keep, half)
    wide = []
    for i in range(2):
        yield ("rs", t, i)
        for s in range(4):
            half = streams[s][1] * 16 >> (i + 1)
            keep = start[s][i + 1]
            flow[s][i].wait_recv()
            mine = scores[pl.ds(keep, half)].astype(jnp.float32)
            mine = mine + landed[pl.ds(slots[4 * i + s], half)].astype(jnp.float32)
            scores[pl.ds(keep, half)] = mine.astype(jnp.bfloat16)
            if i == 0:
                give, _, small = pass_half(s, 1)
                send_half(s, 1, give, small)
            else:
                wide.append(to_three(s, lambda j, flip, to: remote(
                    scores.at[piece(s, flip)], landed.at[corner(s, j)], ws_send.at[j, s], ws_recv.at[j, s], to)))
    yield ("rs", t, 2)
    spread = []
    for s in range(4):
        own = piece(s, (0, 0))
        mine = scores[own].astype(jnp.float32)
        for j in range(3):
            wide[s][j].wait_recv()
            mine = mine + landed[corner(s, j)].astype(jnp.float32)
        scaled[own] = (weights[own] * mine).astype(jnp.bfloat16)
        spread.append(to_three(s, lambda j, flip, to: remote(
            scaled.at[own], scaled.at[own], wg_send.at[j, s], wg_recv.at[j, s], to)))
    back = [[None] * 4 for _ in streams]

    def send_back(s, i):
        half = streams[s][1] * 16 >> (i + 1)
        own = scaled.at[pl.ds(start[s][i + 1], half)]
        back[s][i] = remote(own, own, ag_send.at[i, s], ag_recv.at[i, s], across(s, i))
        back[s][i].start()
        sends.append(back[s][i])

    yield ("ag", t, 0)
    for s in range(4):
        for copy in spread[s]:
            copy.wait_recv()
        send_back(s, 1)
    for i in (1, 0):
        yield ("ag", t, 2 - i)
        for s in range(4):
            back[s][i].wait_recv()
            if i:
                send_back(s, 0)
    total = lax.dot_general(
        scaled[...].reshape(-1, WIDTH), filtered[...], (((0,), (0,)), ((), ())), preferred_element_type=jnp.float32)
    shares[...] = total.reshape(16, 8, -1).astype(jnp.bfloat16)
    swap = remote(shares.at[pl.ds((1 - here.core) * 8, 8)], crossed, d2d_send.at[0], d2d_recv.at[0], here.partner)
    swap.start()
    sends.append(swap)
    yield ("img", t, 0)
    swap.wait_recv()
    rounds = []
    for d in range(1, 8):
        k = (here.z + d) % 8
        pair = shares[here.core * 8 + k].astype(jnp.float32) + crossed[k].astype(jnp.float32)
        halves[d] = pair.astype(jnp.bfloat16)
        copy = remote(halves.at[d], arrived.at[d], z_send.at[d], z_recv.at[d], here.along_z(d))
        copy.start()
        rounds.append(copy)
    sends.extend(rounds)
    own = shares[here.core * 8 + here.z].astype(jnp.float32) + crossed[here.z].astype(jnp.float32)
    yield ("img", t, 1)
    for d, copy in enumerate(rounds, 1):
        copy.wait_recv()
        own = own + arrived[d].astype(jnp.float32)
    mine = here.core * 8 + here.z
    whole[mine] = own.astype(jnp.bfloat16)
    rounds = []
    for d in range(1, 8):
        copy = remote(whole.at[mine], whole.at[mine], g_send.at[d], g_recv.at[d], here.along_z(d))
        copy.start()
        rounds.append(copy)
    sends.extend(rounds)
    over = [remote(whole.at[mine], whole.at[mine], f_send.at[0], f_recv.at[0], here.partner)]
    over[0].start()
    yield ("img", t, 2)
    for d, copy in enumerate(rounds, 1):
        copy.wait_recv()
        k = here.core * 8 + (here.z + 8 - d) % 8
        fwd = remote(whole.at[k], whole.at[k], f_send.at[d], f_recv.at[d], here.partner)
        fwd.start()
        over.append(fwd)
    sends.extend(over)
    yield ("img", t, 3)
    for fwd in over:
        fwd.wait_recv()


def gram_sum(here, sends, basis, out, parts, landed, sems):
    r_send, r_recv, a_send, a_recv = sems
    gram = lax.dot_general(basis[...], basis[...], (((1,), (1,)), ((), ())), preferred_element_type=jnp.float32)
    parts[...] = gram.reshape(16, 16, -1)
    rounds = []
    for d in range(1, 16):
        copy = remote(parts.at[(here.pix + d) % 16], landed.at[d], r_send.at[d], r_recv.at[d], here.in_plane(d))
        copy.start()
        rounds.append(copy)
    sends.extend(rounds)
    own = parts[here.pix]
    yield ("gram", 0, 0)
    for d, copy in enumerate(rounds, 1):
        copy.wait_recv()
        own = own + landed[d]
    out[here.pix] = own
    rounds = []
    for d in range(1, 16):
        copy = remote(out.at[here.pix], out.at[here.pix], a_send.at[d], a_recv.at[d], here.in_plane(d))
        copy.start()
        rounds.append(copy)
    sends.extend(rounds)
    yield ("gram", 0, 1)
    for copy in rounds:
        copy.wait_recv()


def sweeps_kernel(
    images, classes, table, weights, probes, basis, grams,
    filtered, row_weights, first_probe, scores, landed, scaled, shares, crossed, halves, arrived, whole, joined, parts, gram_landed, gram_whole,
    rs_send, rs_recv, ag_send, ag_recv, ws_send, ws_recv, wg_send, wg_recv,
    d2d_send, d2d_recv, z_send, z_recv, g_send, g_recv, f_send, f_recv,
    r_send, r_recv, a_send, a_recv, load_sem,
):
    here = Place()
    loads = []
    for s, (first, share) in enumerate(tiles_of(0)):
        rows = slice(first * 8, (first + 16 * share) * 8)
        loads.append(pltpu.make_async_copy(images.at[rows], filtered.at[rows], load_sem.at[s]))
        loads[-1].start()
    first_probe[...] = probes[...].astype(jnp.bfloat16)
    greet(here)
    sends = []
    all_sems = (
        rs_send, rs_recv, ag_send, ag_recv, ws_send, ws_recv, wg_send, wg_recv,
        d2d_send, d2d_recv, z_send, z_recv, g_send, g_recv, f_send, f_recv)

    def filter_block(b, _):
        rows = pl.ds(pl.multiple_of(b * 128, 128), 128)
        kinds = lax.broadcasted_iota(jnp.int32, (table.shape[0], 128), 0)
        hot = jnp.where(kinds == classes[pl.ds(b, 1), :], 1.0, 0.0).astype(jnp.bfloat16)
        filters = lax.dot_general(hot, table[...], (((0,), (0,)), ((), ())), preferred_element_type=jnp.float32)
        filtered[rows, :] = (filtered[rows, :].astype(jnp.float32) * filters).astype(jnp.bfloat16)
        return 0

    def prepare(s):
        first, share = tiles_of(0)[s]
        loads[s].wait()
        lax.fori_loop(first // 16, first // 16 + share, filter_block, 0)

    def weigh_block(b, _):
        column = jnp.broadcast_to(weights[pl.ds(b, 1), :], (128, 128)).T
        row_weights[pl.ds(b * 16, 16)] = column.reshape(16, 8, 128)
        return 0

    def run(c):
        cols = slice(c * WIDTH, (c + 1) * WIDTH)
        for t in range(ITERS):
            probe = (lambda: first_probe[:, cols]) if t == 0 else (lambda: joined[0, cols, :])
            n = 2 * t + c
            yield from sweep(
                here, sends, t, c, prepare if n == 0 else lambda s: None, filtered, row_weights, probe, scores.at[n], landed.at[n], scaled.at[n], shares.at[n],
                crossed.at[n], halves.at[n], arrived.at[n], whole.at[n], [sem.at[n] for sem in all_sems])
            found = whole[n].reshape(WIDTH, -1)
            if t == 0:
                joined[0, cols, :] = (found.astype(jnp.float32) * DOWN).astype(jnp.bfloat16)
            else:
                basis[cols, :] = found

    def gram(t):
        sems = [sem.at[t] for sem in (r_send, r_recv, a_send, a_recv)]
        yield from gram_sum(
            here, sends, joined.at[0] if t == 0 else basis, gram_whole.at[t], parts.at[t], gram_landed.at[t], sems)

    live = [run(c) for c in range(2)]
    for one in live:
        next(one)
    lax.fori_loop(0, weights.shape[0], weigh_block, 0)
    pending = True
    while live:
        for one in list(live):
            label = next(one, None)
            if label is None:
                live.remove(one)
            elif label == ("img", 1, 0) and pending and one is live[-1]:
                pending = False
                live.append(gram(0))
    for _ in gram(1):
        pass
    grams[...] = gram_whole[...]
    for copy in sends:
        copy.wait_send()


def sweeps(images, classes, table, weights, probes):
    rows, pixels = images.shape
    n = probes.shape[1]
    tiles = rows // 8
    four = 2 * ITERS
    bf16, f32 = jnp.bfloat16, jnp.float32
    dma = pltpu.SemaphoreType.DMA
    vmem = pl.BlockSpec(memory_space=pltpu.VMEM)
    return pl.pallas_call(
        sweeps_kernel,
        out_shape=(jax.ShapeDtypeStruct((n, pixels), bf16), jax.ShapeDtypeStruct((2, 16, 16, n), f32)),
        in_specs=[pl.BlockSpec(memory_space=pl.ANY)] + [vmem] * 4,
        out_specs=[vmem] * 2,
        scratch_shapes=[
            pltpu.VMEM((rows, pixels), bf16),
            pltpu.VMEM((tiles, 8, WIDTH), f32),
            pltpu.VMEM((pixels, n), bf16),
            pltpu.VMEM((four, tiles, 8, WIDTH), bf16),
            pltpu.VMEM((four, tiles * 15 // 16, 8, WIDTH), bf16),
            pltpu.VMEM((four, tiles, 8, WIDTH), bf16),
            pltpu.VMEM((four, 16, 8, pixels), bf16),
            pltpu.VMEM((four, 8, 8, pixels), bf16),
            pltpu.VMEM((four, 8, 8, pixels), bf16),
            pltpu.VMEM((four, 8, 8, pixels), bf16),
            pltpu.VMEM((four, 16, 8, pixels), bf16),
            pltpu.VMEM((1, n, pixels), bf16),
            pltpu.VMEM((2, 16, 16, n), f32),
            pltpu.VMEM((2, 16, 16, n), f32),
            pltpu.VMEM((2, 16, 16, n), f32),
            *[dma((four, 2, 4))] * 4,
            *[dma((four, 3, 4))] * 4,
            *[dma((four, 1))] * 2,
            *[dma((four, 8))] * 6,
            *[dma((2, 16))] * 4,
            dma((4,)),
        ],
        compiler_params=pltpu.CompilerParams(
            collective_id=0, has_side_effects=True, vmem_limit_bytes=56 * 2**20),
    )(images, classes, table, weights, probes)


def per_device(images, classes, ctf_table, weights, probes):
    image_sum, grams = sweeps(images, classes.reshape(-1, 128), ctf_table, weights.reshape(-1, 128), probes)
    n = probes.shape[1]
    return finish(image_sum, grams.reshape(2, n, n))


def solution(mesh):
    return jax.shard_map(
        per_device,
        mesh=mesh,
        in_specs=(P("img", "pix"), P("img"), P(None, "pix"), P("img"), P("pix", None)),
        out_specs=(P("pix", None), P()),
        check_vma=False,
    )
```

```python
import jax
import jax.numpy as jnp
from jax import lax
from jax.experimental import pallas as pl
from jax.experimental.pallas import tpu as pltpu
from jax.sharding import PartitionSpec as P

ITERS = 2

HIGHEST = lax.Precision.HIGHEST
UP = float(2.0**24)
DOWN = float(2.0**-24)

def product(a, b, dims=((1,), (0,))):
    return lax.dot_general(a, b, (dims, ((), ())), precision=HIGHEST, preferred_element_type=jnp.float32)


def split(a):
    top = a.astype(jnp.bfloat16)
    return top, (a - top.astype(jnp.float32)).astype(jnp.bfloat16)


def product3(a, b, dims=((1,), (0,))):
    (a0, a1), (b0, b1) = split(a), split(b)

    def one(p, q):
        return lax.dot_general(p, q, (dims, ((), ())), preferred_element_type=jnp.float32)

    return one(a0, b0) + (one(a0, b1) + one(a1, b0))


def factor_blocks(gram, work, spread, small, inverse, upper):
    pair, n = gram.shape[0], gram.shape[1]
    work[...] = gram[...]
    lane = lax.broadcasted_iota(jnp.int32, (pair, 128), 1)
    col = lax.broadcasted_iota(jnp.int32, (16, n), 1)
    for start in range(0, n, 16):
        chunk = start // 128 * 128
        off = start - chunk
        for g in range(pair):
            block = work[g, start : start + 16, chunk : chunk + 128]
            for j in range(16):
                spread[j, 16 * g : 16 * g + 16, :] = jnp.broadcast_to(block[:, off + j : off + j + 1], (16, 128))
        a = {(i, j): spread[j, pl.ds(i, pair, stride=16), :] for j in range(16) for i in range(j, 16)}
        inv = []
        t = {}
        for j in range(16):
            root = lax.rsqrt(a[j, j])
            inv.append(root)
            for i in range(j + 1, 16):
                a[i, j] = a[i, j] * root
            for m in range(j + 1, 16):
                for i in range(m, 16):
                    a[i, m] = a[i, m] - a[i, j] * a[m, j]
            t[j, j] = root
            row = jnp.where(lane == off + j, root, 0.0)
            for m in range(j):
                total = a[j, m] * t[m, m]
                for q in range(m + 1, j):
                    total = total + a[j, q] * t[q, m]
                t[j, m] = -root * total
                row = jnp.where(lane == off + m, t[j, m], row)
            small[pl.ds(j, pair, stride=16), :] = row
        for g in range(pair):
            head = small[16 * g : 16 * g + 16, :]
            lead = product3(head, work[g, chunk : chunk + 128, :])
            wide = jnp.concatenate([head, head], axis=1) if n == 256 else head
            here = (col >= start) & (col < start + 16)
            mixed = jnp.where(here, wide, lead)
            inverse[g, start : start + 16, :] = jnp.where(col < start + 16, mixed, 0.0)
            upper[g, start : start + 16, :] = jnp.where(
                col >= start + lax.broadcasted_iota(jnp.int32, (16, n), 0), lead, 0.0)
            below = start + 16
            if below < n:
                side = product3(work[g, below:, chunk : chunk + 128], head, ((1,), (1,)))
                cols = lax.broadcasted_iota(jnp.int32, (n - below, n), 1)
                old = work[g, below:, :]
                old = jnp.where((cols >= start) & (cols < below), 0.0, old)
                work[g, below:, :] = old - product3(side, mixed)


def finish_kernel(image_sum, gram, basis, factor, work, spread, small, inverse, upper):
    factor_blocks(gram, work, spread, small, inverse, upper)
    flat = [lax.dot_general(p, image_sum[...], (((1,), (0,)), ((), ())), preferred_element_type=jnp.float32)
            for p in split(inverse[1])]
    basis[...] = (flat[0] + flat[1]).T
    factor[...] = product3(inverse[0], upper[1], ((1,), (1,)))


def finish(image_sum, gram):
    n, rows = image_sum.shape
    return pl.pallas_call(
        finish_kernel,
        out_shape=(jax.ShapeDtypeStruct((rows, n), jnp.float32), jax.ShapeDtypeStruct((n, n), jnp.float32)),
        in_specs=[pl.BlockSpec(memory_space=pltpu.VMEM)] * 2,
        out_specs=[pl.BlockSpec(memory_space=pltpu.VMEM)] * 2,
        scratch_shapes=[
            pltpu.VMEM((2, n, n), jnp.float32),
            pltpu.VMEM((16, 32, 128), jnp.float32),
            pltpu.VMEM((32, 128), jnp.float32),
            pltpu.VMEM((2, n, n), jnp.float32),
            pltpu.VMEM((2, n, n), jnp.float32),
        ],
    )(image_sum, gram)


FLIPS = ((1, 1), (1, 0), (0, 1))
FAR_Z = (4, 3, 5, 2, 6, 1, 7)
FAR_PLANE = tuple(sorted(range(1, 16), key=lambda d: -(min(d // 4, 4 - d // 4) + min(d % 4, 4 - d % 4))))
SHARE_TILES = ((7, 6, 6, 6), (6, 6, 7, 6))
WIDTH = 128
MESH = pl.DeviceIdType.MESH


def remote(src, dst, send, recv, to):
    return pltpu.make_async_remote_copy(
        src_ref=src, dst_ref=dst, send_sem=send, recv_sem=recv, device_id=to, device_id_type=MESH)


class Place:
    def __init__(self):
        self.img, self.pix = lax.axis_index("img"), lax.axis_index("pix")
        self.z, self.core = self.img // 2, self.img % 2
        x, y = self.pix // 4, self.pix % 4
        self.x, self.y = x, y
        self.bits = []
        for near, far in ((x, y), (y, x)):
            high, low = near // 2, near % 2
            self.bits.append(((high + low) % 2, high))
        (xv, xu), (yv, yu) = self.bits
        self.bits = (xv, yv, xu, yu)
        self.flipped = (x + 1 - 2 * (x % 2), y + 1 - 2 * (y % 2), 3 - x, 3 - y)
        self.partner = (self.z * 2 + 1 - self.core, self.pix)

    def across(self, *links):
        x, y = self.x, self.y
        for k in links:
            x, y = (x, self.flipped[k]) if k % 2 else (self.flipped[k], y)
        return (self.img, x * 4 + y)

    def along_z(self, d):
        return ((self.z + d) % 8 * 2 + self.core, self.pix)

    def in_plane(self, d):
        return (self.img, (self.x + d // 4) % 4 * 4 + (self.y + d % 4) % 4)


def greet(here):
    barrier = pltpu.get_barrier_semaphore()
    peers = [here.in_plane(d) for d in range(1, 16)] + [here.along_z(d) for d in range(1, 8)] + [here.partner]
    for peer in peers:
        pl.semaphore_signal(barrier, inc=1, device_id=peer, device_id_type=MESH)
    return lambda: pl.semaphore_wait(barrier, len(peers))


def tiles_of(c):
    first, streams = 0, []
    for share in SHARE_TILES[c]:
        streams.append((first, share))
        first += 16 * share
    return streams


def sweep(here, sends, t, c, prepare, ready, filtered, weights, probe, scores, landed, scaled, shares, crossed, halves, arrived, whole, sems):
    rs_send, rs_recv, ag_send, ag_recv, ws_send, ws_recv, wg_send, wg_recv = sems[:8]
    d2d_send, d2d_recv, z_send, z_recv, g_send, g_recv, f_send, f_recv = sems[8:]
    streams = tiles_of(c)
    dims = ((1,), (0,)) if t == 0 else ((1,), (1,))

    def bit(s, i):
        return here.bits[(s + i) % 4]

    def across(s, i):
        return here.across((s + i) % 4)

    start = [[first] for first, _ in streams]
    flow = [[None] * 4 for _ in streams]
    base = 0

    def score(first, tiles):
        rows = pl.ds(pl.multiple_of(first * 8, 64), tiles * 8)
        part = lax.dot_general(
            filtered[rows, :], probe(), (dims, ((), ())), preferred_element_type=jnp.float32)
        scores[pl.ds(first, tiles)] = part.reshape(tiles, 8, WIDTH).astype(jnp.bfloat16)

    def pass_half(s, i):
        share = streams[s][1]
        half = share * 16 >> (i + 1)
        off = start[s][i]
        give, keep = off + (1 - bit(s, i)) * half, off + bit(s, i) * half
        start[s].append(keep)
        return give, keep, half

    slots = []
    at = 0
    for i in range(2):
        for s in range(4):
            slots.append(at)
            at += streams[s][1] * 16 >> (i + 1)
    for s in range(4):
        slots.append(at)
        at += 3 * streams[s][1]

    def send_half(s, i, give, half):
        flow[s][i] = remote(
            scores.at[pl.ds(give, half)], landed.at[pl.ds(slots[4 * i + s], half)],
            rs_send.at[i, s], rs_recv.at[i, s], across(s, i))
        flow[s][i].start()
        sends.append(flow[s][i])

    def piece(s, flip):
        near, far = (1 - bit(s, i) if f else bit(s, i) for i, f in zip((2, 3), flip))
        return pl.ds(start[s][2] + (2 * near + far) * streams[s][1], streams[s][1])

    def to_three(s, send):
        copies = []
        for j, flip in enumerate(FLIPS):
            links = [(s + i) % 4 for i, f in zip((2, 3), flip) if f]
            copies.append(send(j, flip, here.across(*links)))
            copies[-1].start()
        sends.extend(copies)
        return copies

    def corner(s, j):
        return pl.ds(slots[8 + s] + j * streams[s][1], streams[s][1])

    todo = []
    for s in range(4):
        prepare(s)
        give, keep, half = pass_half(s, 0)
        score(give, half)
        if s == 0:
            ready()
        send_half(s, 0, give, half)
        todo.append((keep, half))
    yield ("keep", t, 0)
    for keep, half in todo:
        score(keep, half)
    wide = []
    for i in range(2):
        yield ("rs", t, i)
        for s in range(4):
            half = streams[s][1] * 16 >> (i + 1)
            keep = start[s][i + 1]
            flow[s][i].wait_recv()
            mine = scores[pl.ds(keep, half)].astype(jnp.float32)
            mine = mine + landed[pl.ds(slots[4 * i + s], half)].astype(jnp.float32)
            scores[pl.ds(keep, half)] = mine.astype(jnp.bfloat16)
            if i == 0:
                give, _, small = pass_half(s, 1)
                send_half(s, 1, give, small)
            else:
                wide.append(to_three(s, lambda j, flip, to: remote(
                    scores.at[piece(s, flip)], landed.at[corner(s, j)], ws_send.at[j, s], ws_recv.at[j, s], to)))
    yield ("rs", t, 2)
    spread = []
    for s in range(4):
        own = piece(s, (0, 0))
        mine = scores[own].astype(jnp.float32)
        for j in range(3):
            wide[s][j].wait_recv()
            mine = mine + landed[corner(s, j)].astype(jnp.float32)
        scaled[own] = (weights[own] * mine).astype(jnp.bfloat16)
        spread.append(to_three(s, lambda j, flip, to: remote(
            scaled.at[own], scaled.at[own], wg_send.at[j, s], wg_recv.at[j, s], to)))
    back = [[None] * 4 for _ in streams]

    def send_back(s, i):
        half = streams[s][1] * 16 >> (i + 1)
        own = scaled.at[pl.ds(start[s][i + 1], half)]
        back[s][i] = remote(own, own, ag_send.at[i, s], ag_recv.at[i, s], across(s, i))
        back[s][i].start()
        sends.append(back[s][i])

    yield ("ag", t, 0)
    for s in range(4):
        for copy in spread[s]:
            copy.wait_recv()
        send_back(s, 1)
    for i in (1, 0):
        yield ("ag", t, 2 - i)
        for s in range(4):
            back[s][i].wait_recv()
            if i:
                send_back(s, 0)
    total = lax.dot_general(
        scaled[...].reshape(-1, WIDTH), filtered[...], (((0,), (0,)), ((), ())), preferred_element_type=jnp.float32)
    shares[...] = total.reshape(16, 8, -1).astype(jnp.bfloat16)
    swap = remote(shares.at[pl.ds((1 - here.core) * 8, 8)], crossed, d2d_send.at[0], d2d_recv.at[0], here.partner)
    swap.start()
    sends.append(swap)
    yield ("img", t, 0)
    swap.wait_recv()
    rounds = {}
    for d in FAR_Z:
        k = (here.z + d) % 8
        pair = shares[here.core * 8 + k].astype(jnp.float32) + crossed[k].astype(jnp.float32)
        halves[d] = pair.astype(jnp.bfloat16)
        copy = remote(halves.at[d], arrived.at[d], z_send.at[d], z_recv.at[d], here.along_z(d))
        copy.start()
        rounds[d] = copy
    sends.extend(rounds.values())
    own = shares[here.core * 8 + here.z].astype(jnp.float32) + crossed[here.z].astype(jnp.float32)
    yield ("img", t, 1)
    for d in FAR_Z[::-1]:
        rounds[d].wait_recv()
        own = own + arrived[d].astype(jnp.float32)
    mine = here.core * 8 + here.z
    whole[mine] = own.astype(jnp.bfloat16)
    rounds = {}
    for d in FAR_Z:
        copy = remote(whole.at[mine], whole.at[mine], g_send.at[d], g_recv.at[d], here.along_z(d))
        copy.start()
        rounds[d] = copy
    sends.extend(rounds.values())
    over = [remote(whole.at[mine], whole.at[mine], f_send.at[0], f_recv.at[0], here.partner)]
    over[0].start()
    yield ("img", t, 2)
    for d in FAR_Z[::-1]:
        rounds[d].wait_recv()
        k = here.core * 8 + (here.z + 8 - d) % 8
        fwd = remote(whole.at[k], whole.at[k], f_send.at[d], f_recv.at[d], here.partner)
        fwd.start()
        over.append(fwd)
    sends.extend(over)
    yield ("img", t, 3)
    for fwd in over:
        fwd.wait_recv()


def gram_sum(here, sends, basis, out, parts, landed, sems):
    r_send, r_recv, a_send, a_recv = sems
    gram = lax.dot_general(basis[...], basis[...], (((1,), (1,)), ((), ())), preferred_element_type=jnp.float32)
    parts[...] = gram.reshape(16, 16, -1)
    rounds = []
    for d in FAR_PLANE:
        copy = remote(parts.at[here.in_plane(d)[1]], landed.at[d], r_send.at[d], r_recv.at[d], here.in_plane(d))
        copy.start()
        rounds.append(copy)
    sends.extend(rounds)
    own = parts[here.pix]
    yield ("gram", 0, 0)
    for d, copy in zip(FAR_PLANE[::-1], rounds[::-1]):
        copy.wait_recv()
        own = own + landed[d]
    out[here.pix] = own
    rounds = []
    for d in FAR_PLANE:
        copy = remote(out.at[here.pix], out.at[here.pix], a_send.at[d], a_recv.at[d], here.in_plane(d))
        copy.start()
        rounds.append(copy)
    sends.extend(rounds)
    yield ("gram", 0, 1)
    for copy in rounds:
        copy.wait_recv()


def sweeps_kernel(
    images, classes, table, weights, probes, basis, grams,
    filtered, row_weights, first_probe, scores, landed, scaled, shares, crossed, halves, arrived, whole, joined, parts, gram_landed, gram_whole,
    rs_send, rs_recv, ag_send, ag_recv, ws_send, ws_recv, wg_send, wg_recv,
    d2d_send, d2d_recv, z_send, z_recv, g_send, g_recv, f_send, f_recv,
    r_send, r_recv, a_send, a_recv, load_sem,
):
    here = Place()
    loads = []
    for s, (first, share) in enumerate(tiles_of(0)):
        rows = slice(first * 8, (first + 16 * share) * 8)
        loads.append(pltpu.make_async_copy(images.at[rows], filtered.at[rows], load_sem.at[s]))
        loads[-1].start()
    first_probe[...] = probes[...].astype(jnp.bfloat16)
    all_here = greet(here)
    sends = []
    all_sems = (
        rs_send, rs_recv, ag_send, ag_recv, ws_send, ws_recv, wg_send, wg_recv,
        d2d_send, d2d_recv, z_send, z_recv, g_send, g_recv, f_send, f_recv)

    def filter_block(b, _):
        rows = pl.ds(pl.multiple_of(b * 128, 128), 128)
        kinds = lax.broadcasted_iota(jnp.int32, (table.shape[0], 128), 0)
        hot = jnp.where(kinds == classes[pl.ds(b, 1), :], 1.0, 0.0).astype(jnp.bfloat16)
        filters = lax.dot_general(hot, table[...], (((0,), (0,)), ((), ())), preferred_element_type=jnp.float32)
        filtered[rows, :] = (filtered[rows, :].astype(jnp.float32) * filters).astype(jnp.bfloat16)
        return 0

    def prepare(s):
        first, share = tiles_of(0)[s]
        loads[s].wait()
        lax.fori_loop(first // 16, first // 16 + share, filter_block, 0)

    def weigh_block(b, _):
        column = jnp.broadcast_to(weights[pl.ds(b, 1), :], (128, 128)).T
        row_weights[pl.ds(b * 16, 16)] = column.reshape(16, 8, 128)
        return 0

    def run(c):
        cols = slice(c * WIDTH, (c + 1) * WIDTH)
        for t in range(ITERS):
            probe = (lambda: first_probe[:, cols]) if t == 0 else (lambda: joined[0, cols, :])
            n = 2 * t + c
            yield from sweep(
                here, sends, t, c, *((prepare, all_here) if n == 0 else (lambda s: None, lambda: None)), filtered, row_weights, probe, scores.at[n], landed.at[n], scaled.at[n], shares.at[n],
                crossed.at[n], halves.at[n], arrived.at[n], whole.at[n], [sem.at[n] for sem in all_sems])
            found = whole[n].reshape(WIDTH, -1)
            if t == 0:
                joined[0, cols, :] = (found.astype(jnp.float32) * DOWN).astype(jnp.bfloat16)
            else:
                basis[cols, :] = found

    def gram(t):
        sems = [sem.at[t] for sem in (r_send, r_recv, a_send, a_recv)]
        yield from gram_sum(
            here, sends, joined.at[0] if t == 0 else basis, gram_whole.at[t], parts.at[t], gram_landed.at[t], sems)

    live = [run(c) for c in range(2)]
    for one in live + live:
        next(one)
    lax.fori_loop(0, weights.shape[0], weigh_block, 0)
    pending = True
    while live:
        for one in list(live):
            label = next(one, None)
            if label is None:
                live.remove(one)
            elif label == ("img", 1, 0) and pending and one is live[-1]:
                pending = False
                live.append(gram(0))
    for _ in gram(1):
        pass
    grams[...] = gram_whole[...]
    for copy in sends:
        copy.wait_send()


def sweeps(images, classes, table, weights, probes):
    rows, pixels = images.shape
    n = probes.shape[1]
    tiles = rows // 8
    four = 2 * ITERS
    bf16, f32 = jnp.bfloat16, jnp.float32
    dma = pltpu.SemaphoreType.DMA
    vmem = pl.BlockSpec(memory_space=pltpu.VMEM)
    return pl.pallas_call(
        sweeps_kernel,
        out_shape=(jax.ShapeDtypeStruct((n, pixels), bf16), jax.ShapeDtypeStruct((2, 16, 16, n), f32)),
        in_specs=[pl.BlockSpec(memory_space=pl.ANY)] + [vmem] * 4,
        out_specs=[vmem] * 2,
        scratch_shapes=[
            pltpu.VMEM((rows, pixels), bf16),
            pltpu.VMEM((tiles, 8, WIDTH), f32),
            pltpu.VMEM((pixels, n), bf16),
            pltpu.VMEM((four, tiles, 8, WIDTH), bf16),
            pltpu.VMEM((four, tiles * 15 // 16, 8, WIDTH), bf16),
            pltpu.VMEM((four, tiles, 8, WIDTH), bf16),
            pltpu.VMEM((four, 16, 8, pixels), bf16),
            pltpu.VMEM((four, 8, 8, pixels), bf16),
            pltpu.VMEM((four, 8, 8, pixels), bf16),
            pltpu.VMEM((four, 8, 8, pixels), bf16),
            pltpu.VMEM((four, 16, 8, pixels), bf16),
            pltpu.VMEM((1, n, pixels), bf16),
            pltpu.VMEM((2, 16, 16, n), f32),
            pltpu.VMEM((2, 16, 16, n), f32),
            pltpu.VMEM((2, 16, 16, n), f32),
            *[dma((four, 2, 4))] * 4,
            *[dma((four, 3, 4))] * 4,
            *[dma((four, 1))] * 2,
            *[dma((four, 8))] * 6,
            *[dma((2, 16))] * 4,
            dma((4,)),
        ],
        compiler_params=pltpu.CompilerParams(
            collective_id=0, has_side_effects=True, vmem_limit_bytes=56 * 2**20),
    )(images, classes, table, weights, probes)


def per_device(images, classes, ctf_table, weights, probes):
    image_sum, grams = sweeps(images, classes.reshape(-1, 128), ctf_table, weights.reshape(-1, 128), probes)
    n = probes.shape[1]
    return finish(image_sum, grams.reshape(2, n, n))


def solution(mesh):
    return jax.shard_map(
        per_device,
        mesh=mesh,
        in_specs=(P("img", "pix"), P("img"), P(None, "pix"), P("img"), P("pix", None)),
        out_specs=(P("pix", None), P()),
        check_vma=False,
    )
```

```python
import jax
import jax.numpy as jnp
from jax import lax
from jax.experimental import pallas as pl
from jax.experimental.pallas import tpu as pltpu
from jax.sharding import PartitionSpec as P

ITERS = 2

DOWN = float(2.0**-24)

def split(a):
    top = a.astype(jnp.bfloat16)
    return top, (a - top.astype(jnp.float32)).astype(jnp.bfloat16)


def product3(a, b, dims=((1,), (0,))):
    (a0, a1), (b0, b1) = split(a), split(b)

    def one(p, q):
        return lax.dot_general(p, q, (dims, ((), ())), preferred_element_type=jnp.float32)

    return one(a0, b0) + (one(a0, b1) + one(a1, b0))


def factor_blocks(gram, work, spread, small, inverse, upper):
    pair, n = gram.shape[0], gram.shape[1]
    work[...] = gram[...]
    lane = lax.broadcasted_iota(jnp.int32, (pair, 128), 1)
    col = lax.broadcasted_iota(jnp.int32, (16, n), 1)
    for start in range(0, n, 16):
        chunk = start // 128 * 128
        off = start - chunk
        for g in range(pair):
            block = work[g, start : start + 16, chunk : chunk + 128]
            for j in range(16):
                spread[j, 16 * g : 16 * g + 16, :] = jnp.broadcast_to(block[:, off + j : off + j + 1], (16, 128))
        a = {}
        t = {}
        for j in range(16):
            for i in range(j, 16):
                entry = spread[j, pl.ds(i, pair, stride=16), :]
                for q in range(j):
                    entry = entry - a[i, q] * a[j, q]
                if i == j:
                    root = lax.rsqrt(entry)
                else:
                    a[i, j] = entry * root
            t[j, j] = root
            row = jnp.where(lane == off + j, root, 0.0)
            for m in range(j):
                total = a[j, m] * t[m, m]
                for q in range(m + 1, j):
                    total = total + a[j, q] * t[q, m]
                t[j, m] = -root * total
                row = jnp.where(lane == off + m, t[j, m], row)
            small[pl.ds(j, pair, stride=16), :] = row
        for g in range(pair):
            head = small[16 * g : 16 * g + 16, :]
            lead = product3(head, work[g, chunk : chunk + 128, :])
            wide = jnp.concatenate([head, head], axis=1) if n == 256 else head
            here = (col >= start) & (col < start + 16)
            mixed = jnp.where(here, wide, lead)
            inverse[g, start : start + 16, :] = jnp.where(col < start + 16, mixed, 0.0)
            upper[g, start : start + 16, :] = jnp.where(
                col >= start + lax.broadcasted_iota(jnp.int32, (16, n), 0), lead, 0.0)
            below = start + 16
            if below < n:
                side = product3(work[g, below:, chunk : chunk + 128], head, ((1,), (1,)))
                cols = lax.broadcasted_iota(jnp.int32, (n - below, n), 1)
                old = work[g, below:, :]
                old = jnp.where((cols >= start) & (cols < below), 0.0, old)
                work[g, below:, :] = old - product3(side, mixed)


def finish_kernel(image_sum, gram, basis, factor, work, spread, small, inverse, upper):
    factor_blocks(gram, work, spread, small, inverse, upper)
    flat = [lax.dot_general(p, image_sum[...], (((1,), (0,)), ((), ())), preferred_element_type=jnp.float32)
            for p in split(inverse[1])]
    basis[...] = (flat[0] + flat[1]).T
    factor[...] = product3(inverse[0], upper[1], ((1,), (1,)))


def finish(image_sum, gram):
    n, rows = image_sum.shape
    return pl.pallas_call(
        finish_kernel,
        out_shape=(jax.ShapeDtypeStruct((rows, n), jnp.float32), jax.ShapeDtypeStruct((n, n), jnp.float32)),
        in_specs=[pl.BlockSpec(memory_space=pltpu.VMEM)] * 2,
        out_specs=[pl.BlockSpec(memory_space=pltpu.VMEM)] * 2,
        scratch_shapes=[
            pltpu.VMEM((2, n, n), jnp.float32),
            pltpu.VMEM((16, 32, 128), jnp.float32),
            pltpu.VMEM((32, 128), jnp.float32),
            pltpu.VMEM((2, n, n), jnp.float32),
            pltpu.VMEM((2, n, n), jnp.float32),
        ],
    )(image_sum, gram)


FLIPS = ((1, 1), (1, 0), (0, 1))
FAR_Z = (4, 3, 5, 2, 6, 1, 7)
FAR_PLANE = tuple(sorted(range(1, 16), key=lambda d: -(min(d // 4, 4 - d // 4) + min(d % 4, 4 - d % 4))))
SHARE_TILES = ((7, 6, 6, 6), (6, 6, 7, 6))
WIDTH = 128
MESH = pl.DeviceIdType.MESH


def remote(src, dst, send, recv, to):
    return pltpu.make_async_remote_copy(
        src_ref=src, dst_ref=dst, send_sem=send, recv_sem=recv, device_id=to, device_id_type=MESH)


class Place:
    def __init__(self):
        self.img, self.pix = lax.axis_index("img"), lax.axis_index("pix")
        self.z, self.core = self.img // 2, self.img % 2
        x, y = self.pix // 4, self.pix % 4
        self.x, self.y = x, y
        self.bits = []
        for near, far in ((x, y), (y, x)):
            high, low = near // 2, near % 2
            self.bits.append(((high + low) % 2, high))
        (xv, xu), (yv, yu) = self.bits
        self.bits = (xv, yv, xu, yu)
        self.flipped = (x + 1 - 2 * (x % 2), y + 1 - 2 * (y % 2), 3 - x, 3 - y)
        self.partner = (self.z * 2 + 1 - self.core, self.pix)

    def across(self, *links):
        x, y = self.x, self.y
        for k in links:
            x, y = (x, self.flipped[k]) if k % 2 else (self.flipped[k], y)
        return (self.img, x * 4 + y)

    def along_z(self, d):
        return ((self.z + d) % 8 * 2 + self.core, self.pix)

    def in_plane(self, d):
        return (self.img, (self.x + d // 4) % 4 * 4 + (self.y + d % 4) % 4)


def greet(here):
    barrier = pltpu.get_barrier_semaphore()
    peers = [here.in_plane(d) for d in range(1, 16)] + [here.along_z(d) for d in range(1, 8)] + [here.partner]
    for peer in peers:
        pl.semaphore_signal(barrier, inc=1, device_id=peer, device_id_type=MESH)
    return lambda: pl.semaphore_wait(barrier, len(peers))


def tiles_of(c):
    first, streams = 0, []
    for share in SHARE_TILES[c]:
        streams.append((first, share))
        first += 16 * share
    return streams


def sweep(here, sends, t, c, prepare, ready, filtered, weights, probe, scores, landed, scaled, shares, crossed, halves, arrived, whole, sems):
    rs_send, rs_recv, ag_send, ag_recv, ws_send, ws_recv, wg_send, wg_recv = sems[:8]
    d2d_send, d2d_recv, z_send, z_recv, g_send, g_recv, f_send, f_recv = sems[8:]
    streams = tiles_of(c)
    dims = ((1,), (0,)) if t == 0 else ((1,), (1,))

    def bit(s, i):
        return here.bits[(s + i) % 4]

    def across(s, i):
        return here.across((s + i) % 4)

    start = [[first] for first, _ in streams]
    flow = [[None] * 4 for _ in streams]
    base = 0

    def score(first, tiles):
        rows = pl.ds(pl.multiple_of(first * 8, 64), tiles * 8)
        part = lax.dot_general(
            filtered[rows, :], probe(), (dims, ((), ())), preferred_element_type=jnp.float32)
        scores[pl.ds(first, tiles)] = part.reshape(tiles, 8, WIDTH).astype(jnp.bfloat16)

    def pass_half(s, i):
        share = streams[s][1]
        half = share * 16 >> (i + 1)
        off = start[s][i]
        give, keep = off + (1 - bit(s, i)) * half, off + bit(s, i) * half
        start[s].append(keep)
        return give, keep, half

    slots = []
    at = 0
    for i in range(2):
        for s in range(4):
            slots.append(at)
            at += streams[s][1] * 16 >> (i + 1)
    for s in range(4):
        slots.append(at)
        at += 3 * streams[s][1]

    def send_half(s, i, give, half):
        flow[s][i] = remote(
            scores.at[pl.ds(give, half)], landed.at[pl.ds(slots[4 * i + s], half)],
            rs_send.at[i, s], rs_recv.at[i, s], across(s, i))
        flow[s][i].start()
        sends.append(flow[s][i])

    def piece(s, flip):
        near, far = (1 - bit(s, i) if f else bit(s, i) for i, f in zip((2, 3), flip))
        return pl.ds(start[s][2] + (2 * near + far) * streams[s][1], streams[s][1])

    def to_three(s, send):
        copies = []
        for j, flip in enumerate(FLIPS):
            links = [(s + i) % 4 for i, f in zip((2, 3), flip) if f]
            copies.append(send(j, flip, here.across(*links)))
            copies[-1].start()
        sends.extend(copies)
        return copies

    def corner(s, j):
        return pl.ds(slots[8 + s] + j * streams[s][1], streams[s][1])

    todo = []
    for s in range(4):
        prepare(s)
        give, keep, half = pass_half(s, 0)
        score(give, half)
        if s == 0:
            ready()
        send_half(s, 0, give, half)
        todo.append((keep, half))
    yield ("keep", t, 0)
    for keep, half in todo:
        score(keep, half)
    wide = []
    for i in range(2):
        yield ("rs", t, i)
        for s in range(4):
            half = streams[s][1] * 16 >> (i + 1)
            keep = start[s][i + 1]
            flow[s][i].wait_recv()
            mine = scores[pl.ds(keep, half)].astype(jnp.float32)
            mine = mine + landed[pl.ds(slots[4 * i + s], half)].astype(jnp.float32)
            scores[pl.ds(keep, half)] = mine.astype(jnp.bfloat16)
            if i == 0:
                give, _, small = pass_half(s, 1)
                send_half(s, 1, give, small)
            else:
                wide.append(to_three(s, lambda j, flip, to: remote(
                    scores.at[piece(s, flip)], landed.at[corner(s, j)], ws_send.at[j, s], ws_recv.at[j, s], to)))
    yield ("rs", t, 2)
    spread = []
    for s in range(4):
        own = piece(s, (0, 0))
        mine = scores[own].astype(jnp.float32)
        for j in range(3):
            wide[s][j].wait_recv()
            mine = mine + landed[corner(s, j)].astype(jnp.float32)
        scaled[own] = (weights[own] * mine).astype(jnp.bfloat16)
        spread.append(to_three(s, lambda j, flip, to: remote(
            scaled.at[own], scaled.at[own], wg_send.at[j, s], wg_recv.at[j, s], to)))
    back = [[None] * 4 for _ in streams]

    def send_back(s, i):
        half = streams[s][1] * 16 >> (i + 1)
        own = scaled.at[pl.ds(start[s][i + 1], half)]
        back[s][i] = remote(own, own, ag_send.at[i, s], ag_recv.at[i, s], across(s, i))
        back[s][i].start()
        sends.append(back[s][i])

    yield ("ag", t, 0)
    for s in range(4):
        for copy in spread[s]:
            copy.wait_recv()
        send_back(s, 1)
    for i in (1, 0):
        yield ("ag", t, 2 - i)
        for s in range(4):
            back[s][i].wait_recv()
            if i:
                send_back(s, 0)
    total = lax.dot_general(
        scaled[...].reshape(-1, WIDTH), filtered[...], (((0,), (0,)), ((), ())), preferred_element_type=jnp.float32)
    shares[...] = total.reshape(16, 8, -1).astype(jnp.bfloat16)
    swap = remote(shares.at[pl.ds((1 - here.core) * 8, 8)], crossed, d2d_send.at[0], d2d_recv.at[0], here.partner)
    swap.start()
    sends.append(swap)
    yield ("img", t, 0)
    swap.wait_recv()
    rounds = {}
    for d in FAR_Z:
        k = (here.z + d) % 8
        pair = shares[here.core * 8 + k].astype(jnp.float32) + crossed[k].astype(jnp.float32)
        halves[d] = pair.astype(jnp.bfloat16)
        copy = remote(halves.at[d], arrived.at[d], z_send.at[d], z_recv.at[d], here.along_z(d))
        copy.start()
        rounds[d] = copy
    sends.extend(rounds.values())
    own = shares[here.core * 8 + here.z].astype(jnp.float32) + crossed[here.z].astype(jnp.float32)
    yield ("img", t, 1)
    for d in FAR_Z[::-1]:
        rounds[d].wait_recv()
        own = own + arrived[d].astype(jnp.float32)
    mine = here.core * 8 + here.z
    whole[mine] = own.astype(jnp.bfloat16)
    rounds = {}
    for d in FAR_Z:
        copy = remote(whole.at[mine], whole.at[mine], g_send.at[d], g_recv.at[d], here.along_z(d))
        copy.start()
        rounds[d] = copy
    sends.extend(rounds.values())
    over = [remote(whole.at[mine], whole.at[mine], f_send.at[0], f_recv.at[0], here.partner)]
    over[0].start()
    yield ("img", t, 2)
    for d in FAR_Z[::-1]:
        rounds[d].wait_recv()
        k = here.core * 8 + (here.z + 8 - d) % 8
        fwd = remote(whole.at[k], whole.at[k], f_send.at[d], f_recv.at[d], here.partner)
        fwd.start()
        over.append(fwd)
    sends.extend(over)
    yield ("img", t, 3)
    for fwd in over:
        fwd.wait_recv()


def gram_sum(here, sends, basis, out, parts, landed, sems):
    r_send, r_recv, a_send, a_recv = sems
    gram = lax.dot_general(basis[...], basis[...], (((1,), (1,)), ((), ())), preferred_element_type=jnp.float32)
    parts[...] = gram.reshape(16, 16, -1)
    rounds = []
    for d in FAR_PLANE:
        copy = remote(parts.at[here.in_plane(d)[1]], landed.at[d], r_send.at[d], r_recv.at[d], here.in_plane(d))
        copy.start()
        rounds.append(copy)
    sends.extend(rounds)
    own = parts[here.pix]
    yield ("gram", 0, 0)
    for d, copy in zip(FAR_PLANE[::-1], rounds[::-1]):
        copy.wait_recv()
        own = own + landed[d]
    out[here.pix] = own
    rounds = []
    for d in FAR_PLANE:
        copy = remote(out.at[here.pix], out.at[here.pix], a_send.at[d], a_recv.at[d], here.in_plane(d))
        copy.start()
        rounds.append(copy)
    sends.extend(rounds)
    yield ("gram", 0, 1)
    for copy in rounds:
        copy.wait_recv()


def sweeps_kernel(
    images, classes, table, weights, probes, basis, grams,
    filtered, row_weights, first_probe, scores, landed, scaled, shares, crossed, halves, arrived, whole, joined, parts, gram_landed, gram_whole,
    rs_send, rs_recv, ag_send, ag_recv, ws_send, ws_recv, wg_send, wg_recv,
    d2d_send, d2d_recv, z_send, z_recv, g_send, g_recv, f_send, f_recv,
    r_send, r_recv, a_send, a_recv, load_sem,
):
    here = Place()
    all_here = greet(here)
    loads = []
    for s, (first, share) in enumerate(tiles_of(0)):
        rows = slice(first * 8, (first + 16 * share) * 8)
        loads.append(pltpu.make_async_copy(images.at[rows], filtered.at[rows], load_sem.at[s]))
        loads[-1].start()
    first_probe[...] = probes[...].astype(jnp.bfloat16)
    sends = []
    all_sems = (
        rs_send, rs_recv, ag_send, ag_recv, ws_send, ws_recv, wg_send, wg_recv,
        d2d_send, d2d_recv, z_send, z_recv, g_send, g_recv, f_send, f_recv)

    def filter_block(b, _):
        rows = pl.ds(pl.multiple_of(b * 128, 128), 128)
        kinds = lax.broadcasted_iota(jnp.int32, (table.shape[0], 128), 0)
        hot = jnp.where(kinds == classes[pl.ds(b, 1), :], 1.0, 0.0).astype(jnp.bfloat16)
        filters = lax.dot_general(hot, table[...], (((0,), (0,)), ((), ())), preferred_element_type=jnp.float32)
        filtered[rows, :] = (filtered[rows, :].astype(jnp.float32) * filters).astype(jnp.bfloat16)
        return 0

    def prepare(s):
        first, share = tiles_of(0)[s]
        loads[s].wait()
        lax.fori_loop(first // 16, first // 16 + share, filter_block, 0)

    def weigh_block(b, _):
        column = jnp.broadcast_to(weights[pl.ds(b, 1), :], (128, 128)).T
        row_weights[pl.ds(b * 16, 16)] = column.reshape(16, 8, 128)
        return 0

    def run(c):
        cols = slice(c * WIDTH, (c + 1) * WIDTH)
        for t in range(ITERS):
            probe = (lambda: first_probe[:, cols]) if t == 0 else (lambda: joined[0, cols, :])
            n = 2 * t + c
            yield from sweep(
                here, sends, t, c, *((prepare, all_here) if n == 0 else (lambda s: None, lambda: None)), filtered, row_weights, probe, scores.at[n], landed.at[n], scaled.at[n], shares.at[n],
                crossed.at[n], halves.at[n], arrived.at[n], whole.at[n], [sem.at[n] for sem in all_sems])
            found = whole[n].reshape(WIDTH, -1)
            if t == 0:
                joined[0, cols, :] = (found.astype(jnp.float32) * DOWN).astype(jnp.bfloat16)
            else:
                basis[cols, :] = found

    def gram(t):
        sems = [sem.at[t] for sem in (r_send, r_recv, a_send, a_recv)]
        yield from gram_sum(
            here, sends, joined.at[0] if t == 0 else basis, gram_whole.at[t], parts.at[t], gram_landed.at[t], sems)

    live = [run(c) for c in range(2)]
    for one in live + live:
        next(one)
    lax.fori_loop(0, weights.shape[0], weigh_block, 0)
    pending = True
    while live:
        for one in list(live):
            label = next(one, None)
            if label is None:
                live.remove(one)
            elif label == ("img", 1, 0) and pending and one is live[-1]:
                pending = False
                live.append(gram(0))
    for _ in gram(1):
        pass
    grams[...] = gram_whole[...]
    for copy in sends:
        copy.wait_send()


def sweeps(images, classes, table, weights, probes):
    rows, pixels = images.shape
    n = probes.shape[1]
    tiles = rows // 8
    four = 2 * ITERS
    bf16, f32 = jnp.bfloat16, jnp.float32
    dma = pltpu.SemaphoreType.DMA
    vmem = pl.BlockSpec(memory_space=pltpu.VMEM)
    return pl.pallas_call(
        sweeps_kernel,
        out_shape=(jax.ShapeDtypeStruct((n, pixels), bf16), jax.ShapeDtypeStruct((2, 16, 16, n), f32)),
        in_specs=[pl.BlockSpec(memory_space=pl.ANY)] + [vmem] * 4,
        out_specs=[vmem] * 2,
        scratch_shapes=[
            pltpu.VMEM((rows, pixels), bf16),
            pltpu.VMEM((tiles, 8, WIDTH), f32),
            pltpu.VMEM((pixels, n), bf16),
            pltpu.VMEM((four, tiles, 8, WIDTH), bf16),
            pltpu.VMEM((four, tiles * 15 // 16, 8, WIDTH), bf16),
            pltpu.VMEM((four, tiles, 8, WIDTH), bf16),
            pltpu.VMEM((four, 16, 8, pixels), bf16),
            pltpu.VMEM((four, 8, 8, pixels), bf16),
            pltpu.VMEM((four, 8, 8, pixels), bf16),
            pltpu.VMEM((four, 8, 8, pixels), bf16),
            pltpu.VMEM((four, 16, 8, pixels), bf16),
            pltpu.VMEM((1, n, pixels), bf16),
            pltpu.VMEM((2, 16, 16, n), f32),
            pltpu.VMEM((2, 16, 16, n), f32),
            pltpu.VMEM((2, 16, 16, n), f32),
            *[dma((four, 2, 4))] * 4,
            *[dma((four, 3, 4))] * 4,
            *[dma((four, 1))] * 2,
            *[dma((four, 8))] * 6,
            *[dma((2, 16))] * 4,
            dma((4,)),
        ],
        compiler_params=pltpu.CompilerParams(
            collective_id=0, has_side_effects=True, vmem_limit_bytes=56 * 2**20),
    )(images, classes, table, weights, probes)


def per_device(images, classes, ctf_table, weights, probes):
    image_sum, grams = sweeps(images, classes.reshape(-1, 128), ctf_table, weights.reshape(-1, 128), probes)
    n = probes.shape[1]
    return finish(image_sum, grams.reshape(2, n, n))


def solution(mesh):
    return jax.shard_map(
        per_device,
        mesh=mesh,
        in_specs=(P("img", "pix"), P("img"), P(None, "pix"), P("img"), P("pix", None)),
        out_specs=(P("pix", None), P()),
        check_vma=False,
    )
```
